256 devices in a mesh: shard: 64 (over z, x, core), model: 4 (over y).
Axes of the slice: x: 4, y: 4, z: 8, core: 2. Of those that a mesh axis runs over, the one named last changes fastest.
Arguments:
- grad_stack: float32 [512, 128, 2048], P(None, 'shard', 'model'), may hold values from -6 to 6
- moment_stack: float32 [512, 128, 2048], P(None, 'shard', 'model'), may hold values from -6 to 6
- weight_stack: float32 [512, 128, 2048], P(None, 'shard', 'model'), may hold values from -0.1875 to 0.1875
Outputs:
- new_weights: float32 [512, 128, 2048], P(None, 'shard', 'model')
- new_momentum: float32 [512, 128, 2048], P(None, 'shard', 'model')
The draws below stay inside these ranges and needn't reach their ends.
All inputs are finite; a program needn't handle non-finite values.
Results may differ from the reference program's by a relative error of at most 0.00021.
Values sent between devices are 32-bit elements; how exact they have to be, the bound alone decides.
A program may use at most 64 MiB of HBM per device.

```python
import jax
import jax.numpy as jnp
from jax import lax

SIDE = 128
WIDE = 2048
MATS = 512
ITERS = 5


def shard_levels(own_key, extent, pieces, least, high):
    def one(position, parts):
        steps = jax.random.uniform(jax.random.fold_in(jax.random.fold_in(own_key, 6), position), (parts,), jnp.float32, least / len(pieces), high / len(pieces))
        return jnp.repeat(jnp.exp(steps), extent[position] // parts).reshape((-1,) + (1,) * (len(extent) - position - 1))

    loudness = one(*pieces[0])
    for cut in pieces[1:]:
        loudness = loudness * one(*cut)
    return loudness


def noise(rng, extent, width, most, shards=(), held_as=jnp.bfloat16):
    drawn = jax.random.normal(rng, extent, jnp.float32) * width
    if len(shards) > 0:
        drawn = shard_levels(rng, extent, shards, -0.22, 0.18) * drawn
    return jnp.clip(drawn, min=-most, max=most).astype(held_as)


def setup_inputs(seed: int = 0) -> dict:
    key_list = jax.random.split(jax.random.key(seed), 4)
    grad_stack = noise(key_list[0], (MATS, SIDE, WIDE), 1.0, 6.0, ((1, 64), (2, 4)), jnp.float32)
    moment_stack = noise(key_list[1], (MATS, SIDE, WIDE), 1.0, 6.0, ((1, 64), (2, 4)), jnp.float32)
    weight_stack = noise(key_list[2], (MATS, SIDE, WIDE), 0.03, 0.1875, ((1, 64), (2, 4)), jnp.float32)
    return {"grad_stack": grad_stack, "moment_stack": moment_stack, "weight_stack": weight_stack}


hold_rate = 0.95
learn_rate = 1.0
decay_rate = 0.1

def reference(grad_stack, moment_stack, weight_stack):
    new_momentum = hold_rate * moment_stack + grad_stack

    def orthogonal_one(stack):
        iterate = stack[None]
        iterate = iterate * lax.rsqrt(lax.optimization_barrier(jnp.sum(iterate * iterate, axis=(1, 2), keepdims=True)) + 1e-06)
        for step in range(ITERS):
            gram = jnp.einsum('mik,mjk->mij', iterate, iterate, precision=lax.Precision.HIGHEST)
            mixed = -4.775 * gram + 2.0315 * jnp.einsum('mij,mjk->mik', gram, gram, precision=lax.Precision.HIGHEST)
            iterate = 3.4445 * iterate + jnp.einsum('mij,mjk->mik', mixed, iterate, precision=lax.Precision.HIGHEST)
        return iterate[0]
    iterate = lax.map(orthogonal_one, new_momentum)
    new_weights = (1.0 - learn_rate * decay_rate) * weight_stack - learn_rate * iterate
    return (new_weights, new_momentum)
```

```python
import jax
import jax.numpy as jnp
from jax import lax
from jax.sharding import PartitionSpec as P

hold_rate = 0.95
learn_rate = 1.0
decay_rate = 0.1
HIGH = lax.Precision.HIGHEST


def mul(a, b):
    return jnp.einsum("mij,mjk->mik", a, b, precision=HIGH)


def chain(gram, steps):
    eye = jnp.eye(gram.shape[-1], dtype=gram.dtype)
    total = None
    for step in range(steps):
        factor = 3.4445 * eye - 4.775 * gram + 2.0315 * mul(gram, gram)
        total = factor if total is None else mul(factor, total)
        if step < steps - 1:
            gram = mul(mul(factor, gram), factor)
    return total


def summed_gram(rows):
    part = jnp.einsum("mik,mjk->mij", rows, rows, precision=HIGH)
    parts = lax.all_to_all(part, "model", split_axis=0, concat_axis=0, tiled=True)
    return parts.reshape(4, -1, *parts.shape[1:]).sum(axis=0)


def on_device(grad_stack, moment_stack, weight_stack):
    new_momentum = hold_rate * moment_stack + grad_stack
    rows = lax.all_to_all(new_momentum, "shard", split_axis=0, concat_axis=1, tiled=True)
    gram = summed_gram(rows)
    scale = lax.rsqrt(jnp.trace(gram, axis1=1, axis2=2)[:, None, None] + 1e-06)
    first = chain(gram * scale * scale, 2) * scale
    rows = mul(lax.all_gather(first, "model", axis=0, tiled=True), rows)
    second = chain(summed_gram(rows), 3)
    rows = mul(lax.all_gather(second, "model", axis=0, tiled=True), rows)
    back = lax.all_to_all(rows, "shard", split_axis=1, concat_axis=0, tiled=True)
    new_weights = (1.0 - learn_rate * decay_rate) * weight_stack - learn_rate * back
    return (new_weights, new_momentum)


def solution(mesh):
    spec = P(None, "shard", "model")
    return jax.shard_map(on_device, mesh=mesh, in_specs=(spec,) * 3, out_specs=(spec,) * 2, check_vma=False)
```

```python
import functools

import jax
import jax.numpy as jnp
from jax import lax
from jax.experimental import pallas as pl
from jax.experimental.pallas import tpu as pltpu
from jax.sharding import PartitionSpec as P

hold_rate = 0.95
learn_rate = 1.0
decay_rate = 0.1
HIGH = lax.Precision.HIGHEST
MESH = pl.DeviceIdType.MESH
F32 = jnp.float32

LANES = 128
TILE = 8
PAIR = 2
ROWS = PAIR * TILE


def mul(a, b):
    return lax.dot_general(a, b, (((1,), (0,)), ((), ())), precision=HIGH, preferred_element_type=F32)


def gram_of(x):
    return lax.dot_general(x, x, (((1,), (1,)), ((), ())), precision=HIGH, preferred_element_type=F32)


def diagonal(side):
    return lax.broadcasted_iota(jnp.int32, (side, side), 0) == lax.broadcasted_iota(jnp.int32, (side, side), 1)


def chain(grams, steps):
    eye = jnp.where(diagonal(grams[0].shape[0]), 3.4445, 0.0).astype(F32)
    totals = None
    for step in range(steps):
        squares = [mul(a, a) for a in grams]
        factors = [eye - 4.775 * a + 2.0315 * s for a, s in zip(grams, squares)]
        totals = factors if totals is None else [mul(f, t) for f, t in zip(factors, totals)]
        if step < steps - 1:
            half = [mul(f, a) for f, a in zip(factors, grams)]
            grams = [mul(h, f) for h, f in zip(half, factors)]
    return totals


def exchange_kernel(
    shards, models, chunks,
    grad, moment, back, held,
    grad_in, moment_in, rows, whole, moved, out, grams,
    in_sem, go_send, go_recv, gram_send, gram_recv, home_send, home_recv,
):
    me, mine = lax.axis_index("shard"), lax.axis_index("model")
    side = 2 * shards
    barrier = pltpu.get_barrier_semaphore()

    loads = [
        pltpu.make_async_copy(grad, grad_in, in_sem.at[0]),
        pltpu.make_async_copy(moment, moment_in, in_sem.at[1]),
    ]
    for load in loads:
        load.start()

    @pl.loop(1, shards)
    def _(step):
        pl.semaphore_signal(barrier, inc=1, device_id=(lax.rem(me + step, shards), mine), device_id_type=MESH)

    for step in range(1, models):
        pl.semaphore_signal(barrier, inc=1, device_id=(me, lax.rem(mine + step, models)), device_id_type=MESH)

    for load in loads:
        load.wait()

    @pl.loop(0, shards)
    def _(peer):
        held[peer] = hold_rate * moment_in[peer] + grad_in[peer]

    pl.semaphore_wait(barrier, shards - 1 + models - 1)

    def slot(peer):
        return pl.ds(pl.multiple_of(peer * ROWS, ROWS), ROWS)

    @pl.loop(0, chunks)
    def _(chunk):
        @pl.loop(1, shards)
        def _(step):
            peer = lax.rem(me + step, shards)
            pltpu.make_async_remote_copy(
                src_ref=held.at[peer, chunk], dst_ref=rows.at[chunk, slot(me)],
                send_sem=go_send, recv_sem=go_recv.at[chunk],
                device_id=(peer, mine), device_id_type=MESH,
            ).start()

        rows[chunk, slot(me)] = held[me, chunk]

    def landed(chunk):
        part = rows.at[chunk, pl.ds(0, (shards - 1) * ROWS)]
        return part

    def share_gram(turn, chunk):
        for step in range(1, models):
            peer = lax.rem(mine + step, models)
            pltpu.make_async_remote_copy(
                src_ref=grams.at[turn, chunk, mine], dst_ref=grams.at[turn, chunk, mine],
                send_sem=gram_send, recv_sem=gram_recv.at[turn, chunk],
                device_id=(me, peer), device_id_type=MESH,
            ).start()

    def summed_grams(turn, chunk):
        part = grams.at[turn, chunk, pl.ds(0, models - 1)]
        pltpu.make_async_copy(part, part, gram_recv.at[turn, chunk]).wait()
        sums = []
        for i in range(PAIR):
            total = grams[turn, chunk, 0, i]
            for k in range(1, models):
                total = total + grams[turn, chunk, k, i]
            sums.append(total)
        return sums

    def first_stage(chunk):
        part = landed(chunk)
        pltpu.make_async_copy(part, part, go_recv.at[chunk]).wait()
        for i in range(PAIR):
            for c in range(TILE // 2):
                for r in range(2):
                    whole[chunk, i, pl.ds(r * shards, shards), pl.ds(c * LANES, LANES)] = rows[
                        chunk, pl.ds(i * TILE + 2 * c + r, shards, stride=ROWS), :
                    ]
        for i in range(PAIR):
            grams[0, chunk, mine, i] = gram_of(whole[chunk, i])
        share_gram(0, chunk)

    def second_stage(chunk):
        sums = summed_grams(0, chunk)
        mask = diagonal(side)
        scales = [
            lax.rsqrt(jnp.sum(jnp.sum(jnp.where(mask, g, 0.0), axis=1, keepdims=True), axis=0, keepdims=True) + 1e-06)
            for g in sums
        ]
        factors = chain([g * s * s for g, s in zip(sums, scales)], 2)
        for i in range(PAIR):
            moved[chunk, i] = mul(factors[i] * scales[i], whole[chunk, i])
        for i in range(PAIR):
            grams[1, chunk, mine, i] = gram_of(moved[chunk, i])
        share_gram(1, chunk)

    def third_stage(chunk):
        factors = chain(summed_grams(1, chunk), 3)
        for i in range(PAIR):
            final = mul(factors[i], moved[chunk, i])
            for c in range(TILE // 2):
                for r in range(2):
                    out[chunk, pl.ds(i * TILE + 2 * c + r, shards, stride=ROWS), :] = final[
                        r * shards : (r + 1) * shards, c * LANES : (c + 1) * LANES
                    ]

        @pl.loop(1, shards)
        def _(step):
            peer = lax.rem(me + step, shards)
            pltpu.make_async_remote_copy(
                src_ref=out.at[chunk, slot(peer)], dst_ref=back.at[me, chunk],
                send_sem=home_send, recv_sem=home_recv,
                device_id=(peer, mine), device_id_type=MESH,
            ).start()

        back[me, chunk] = out[chunk, slot(me)]

    @pl.loop(0, chunks)
    def _(chunk):
        first_stage(chunk)

        @pl.when(chunk > 0)
        def _():
            third_stage(chunk - 1)

        second_stage(chunk)

    third_stage(chunks - 1)

    part = back.at[pl.ds(0, shards - 1)]
    pltpu.make_async_copy(part, part, home_recv).wait()
    pltpu.make_async_copy(part, part, home_send).wait()
    pltpu.make_async_copy(part, part, go_send).wait()
    part = grams.at[:, :, pl.ds(0, models - 1)]
    pltpu.make_async_copy(part, part, gram_send).wait()


def finish_kernel(back, held, weight, new_weights, new_momentum, result, sems):
    first = pltpu.make_async_copy(held, new_momentum, sems.at[0])
    first.start()

    @pl.loop(0, back.shape[0])
    def _(peer):
        result[peer] = (1.0 - learn_rate * decay_rate) * weight[peer] - learn_rate * back[peer]

    last = pltpu.make_async_copy(result, new_weights, sems.at[1])
    last.start()
    last.wait()
    first.wait()


def solution(mesh):
    shards, models = mesh.shape["shard"], mesh.shape["model"]

    def folded(x):
        mats, two, wide = x.shape
        x = x.reshape(mats, two, wide // LANES, LANES).transpose(0, 2, 1, 3)
        return x.reshape(shards, mats // (shards * PAIR), ROWS, LANES)

    def unfolded(x, like):
        mats, two, wide = like.shape
        x = x.reshape(mats, wide // LANES, two, LANES).transpose(0, 2, 1, 3)
        return x.reshape(like.shape)

    def on_device(grad_stack, moment_stack, weight_stack):
        grad, moment, weight = folded(grad_stack), folded(moment_stack), folded(weight_stack)
        shape = grad.shape
        chunks = shape[1]
        side, wide = 2 * shards, TILE // 2 * LANES
        vmem = pl.BlockSpec(memory_space=pltpu.VMEM)
        far = pl.BlockSpec(memory_space=pltpu.HBM)
        block = jax.ShapeDtypeStruct(shape, F32)
        back, held = pl.pallas_call(
            functools.partial(exchange_kernel, shards, models, chunks),
            name="exchange",
            out_shape=(block, block),
            in_specs=[far, far],
            out_specs=(vmem, vmem),
            scratch_shapes=[
                pltpu.VMEM(shape, F32),
                pltpu.VMEM(shape, F32),
                pltpu.VMEM((chunks, shards * ROWS, LANES), F32),
                pltpu.VMEM((chunks, PAIR, side, wide), F32),
                pltpu.VMEM((chunks, PAIR, side, wide), F32),
                pltpu.VMEM((chunks, shards * ROWS, LANES), F32),
                pltpu.VMEM((2, chunks, models, PAIR, side, side), F32),
                pltpu.SemaphoreType.DMA((2,)),
                pltpu.SemaphoreType.DMA,
                pltpu.SemaphoreType.DMA((chunks,)),
                pltpu.SemaphoreType.DMA,
                pltpu.SemaphoreType.DMA((2, chunks)),
                pltpu.SemaphoreType.DMA,
                pltpu.SemaphoreType.DMA,
            ],
            compiler_params=pltpu.CompilerParams(
                collective_id=0, has_side_effects=True, vmem_limit_bytes=40 * 1024 * 1024
            ),
        )(grad, moment)
        new_weights, new_momentum = pl.pallas_call(
            finish_kernel,
            name="finish",
            out_shape=(block, block),
            in_specs=[vmem, vmem, vmem],
            out_specs=(far, far),
            scratch_shapes=[pltpu.VMEM(shape, F32), pltpu.SemaphoreType.DMA((2,))],
            compiler_params=pltpu.CompilerParams(vmem_limit_bytes=16 * 1024 * 1024),
        )(back, held, weight)
        return unfolded(new_weights, weight_stack), unfolded(new_momentum, weight_stack)

    spec = P(None, "shard", "model")
    return jax.shard_map(on_device, mesh=mesh, in_specs=(spec,) * 3, out_specs=(spec,) * 2, check_vma=False)
```

```python
import functools

import jax
import jax.numpy as jnp
from jax import lax
from jax.experimental import pallas as pl
from jax.experimental.pallas import tpu as pltpu
from jax.sharding import PartitionSpec as P

hold_rate = 0.95
learn_rate = 1.0
decay_rate = 0.1
HIGH = lax.Precision.HIGHEST
MESH = pl.DeviceIdType.MESH
F32 = jnp.float32

LANES = 128
TILE = 8
PAIR = 2
ROWS = PAIR * TILE


def mul(a, b):
    return lax.dot_general(a, b, (((1,), (0,)), ((), ())), precision=HIGH, preferred_element_type=F32)


def gram_of(x):
    return lax.dot_general(x, x, (((1,), (1,)), ((), ())), precision=HIGH, preferred_element_type=F32)


def diagonal(side):
    return lax.broadcasted_iota(jnp.int32, (side, side), 0) == lax.broadcasted_iota(jnp.int32, (side, side), 1)


def chain(grams, steps):
    eye = jnp.where(diagonal(grams[0].shape[0]), 3.4445, 0.0).astype(F32)
    totals = None
    for step in range(steps):
        squares = [mul(a, a) for a in grams]
        factors = [eye - 4.775 * a + 2.0315 * s for a, s in zip(grams, squares)]
        totals = factors if totals is None else [mul(f, t) for f, t in zip(factors, totals)]
        if step < steps - 1:
            half = [mul(f, a) for f, a in zip(factors, grams)]
            grams = [mul(h, f) for h, f in zip(half, factors)]
    return totals


def peers_in_order(me, shards):
    depth, flat = shards // 8, 8
    z, rest = me // flat, lax.rem(me, flat)
    x, core = rest // 2, lax.rem(rest, 2)
    around = [0] + [d for k in range(1, depth) for d in (k, depth - k)][: depth - 1]
    around = around[1:] + around[:1]
    zs = [lax.rem(z + d, depth) * flat for d in around]
    xs = [lax.rem(x + dx, 4) * 2 + lax.rem(core + dc, 2) for dx in (0, 1, 3, 2) for dc in (0, 1)]
    order = [(zs[(i + j) % depth], xs[j], around[(i + j) % depth], j) for i in range(depth) for j in range(flat)]
    return [a + b for a, b, d, j in order if (d, j) != (0, 0)]


def exchange_kernel(
    shards, models, chunks,
    grad, moment, weight, fresh, held,
    grad_in, moment_in, weight_in, rows, whole, moved, out, back, grams,
    in_sem, go_send, go_recv, gram_send, gram_recv, home_send, home_recv,
):
    me, mine = lax.axis_index("shard"), lax.axis_index("model")
    side = 2 * shards
    barrier = pltpu.get_barrier_semaphore()
    peers = peers_in_order(me, shards)
    others = [lax.rem(mine + step, models) for step in range(1, models)]

    for peer in peers:
        pl.semaphore_signal(barrier, inc=1, device_id=(peer, mine), device_id_type=MESH)
    for other in others:
        pl.semaphore_signal(barrier, inc=1, device_id=(me, other), device_id_type=MESH)

    def load(source, target, which, chunk):
        return pltpu.make_async_copy(source.at[:, chunk], target.at[:, chunk], in_sem.at[which, chunk])

    for chunk in range(chunks):
        load(grad, grad_in, 0, chunk).start()
        load(moment, moment_in, 1, chunk).start()
    for chunk in range(chunks):
        load(grad, grad_in, 0, chunk).wait()
        load(moment, moment_in, 1, chunk).wait()
        held[:, chunk] = hold_rate * moment_in[:, chunk] + grad_in[:, chunk]

    pl.semaphore_wait(barrier, len(peers) + len(others))

    def slot(peer):
        return pl.ds(pl.multiple_of(peer * ROWS, ROWS), ROWS)

    @pl.loop(0, chunks)
    def _(chunk):
        for peer in peers:
            pltpu.make_async_remote_copy(
                src_ref=held.at[peer, chunk], dst_ref=rows.at[chunk, slot(me)],
                send_sem=go_send, recv_sem=go_recv.at[chunk],
                device_id=(peer, mine), device_id_type=MESH,
            ).start()
        rows[chunk, slot(me)] = held[me, chunk]

    for chunk in range(chunks):
        load(weight, weight_in, 2, chunk).start()

    def landed(chunk):
        return rows.at[chunk, pl.ds(0, (shards - 1) * ROWS)]

    def share_gram(turn, chunk):
        for other in others:
            pltpu.make_async_remote_copy(
                src_ref=grams.at[turn, chunk, mine], dst_ref=grams.at[turn, chunk, mine],
                send_sem=gram_send, recv_sem=gram_recv.at[turn, chunk],
                device_id=(me, other), device_id_type=MESH,
            ).start()

    def summed_grams(turn, chunk):
        part = grams.at[turn, chunk, pl.ds(0, models - 1)]
        pltpu.make_async_copy(part, part, gram_recv.at[turn, chunk]).wait()
        sums = []
        for i in range(PAIR):
            total = grams[turn, chunk, 0, i]
            for k in range(1, models):
                total = total + grams[turn, chunk, k, i]
            sums.append(total)
        return sums

    def first_stage(chunk):
        part = landed(chunk)
        pltpu.make_async_copy(part, part, go_recv.at[chunk]).wait()
        for i in range(PAIR):
            for c in range(TILE // 2):
                for r in range(2):
                    whole[chunk, i, pl.ds(r * shards, shards), pl.ds(c * LANES, LANES)] = rows[
                        chunk, pl.ds(i * TILE + 2 * c + r, shards, stride=ROWS), :
                    ]
        for i in range(PAIR):
            grams[0, chunk, mine, i] = gram_of(whole[chunk, i])
        share_gram(0, chunk)

    def second_stage(chunk):
        sums = summed_grams(0, chunk)
        mask = diagonal(side)
        scales = [
            lax.rsqrt(jnp.sum(jnp.sum(jnp.where(mask, g, 0.0), axis=1, keepdims=True), axis=0, keepdims=True) + 1e-06)
            for g in sums
        ]
        factors = chain([g * s * s for g, s in zip(sums, scales)], 2)
        for i in range(PAIR):
            moved[chunk, i] = mul(factors[i] * scales[i], whole[chunk, i])
        for i in range(PAIR):
            grams[1, chunk, mine, i] = gram_of(moved[chunk, i])
        share_gram(1, chunk)

    def third_stage(chunk):
        factors = chain(summed_grams(1, chunk), 3)
        for i in range(PAIR):
            final = mul(factors[i], moved[chunk, i])
            for c in range(TILE // 2):
                for r in range(2):
                    out[chunk, pl.ds(i * TILE + 2 * c + r, shards, stride=ROWS), :] = final[
                        r * shards : (r + 1) * shards, c * LANES : (c + 1) * LANES
                    ]

        for peer in peers:
            pltpu.make_async_remote_copy(
                src_ref=out.at[chunk, slot(peer)], dst_ref=back.at[chunk, slot(me)],
                send_sem=home_send, recv_sem=home_recv.at[chunk],
                device_id=(peer, mine), device_id_type=MESH,
            ).start()
        back[chunk, slot(me)] = out[chunk, slot(me)]

    @pl.loop(0, chunks)
    def _(chunk):
        first_stage(chunk)

        @pl.when(chunk > 0)
        def _():
            third_stage(chunk - 1)

        second_stage(chunk)

    third_stage(chunks - 1)

    for chunk in range(chunks):
        load(weight, weight_in, 2, chunk).wait()
        part = back.at[chunk, pl.ds(0, (shards - 1) * ROWS)]
        pltpu.make_async_copy(part, part, home_recv.at[chunk]).wait()
        fresh[:, chunk] = (1.0 - learn_rate * decay_rate) * weight_in[:, chunk] - learn_rate * back[chunk].reshape(
            shards, ROWS, LANES
        )

    part = held.at[pl.ds(0, shards - 1)]
    pltpu.make_async_copy(part, part, home_send).wait()
    pltpu.make_async_copy(part, part, go_send).wait()
    part = grams.at[:, :, pl.ds(0, models - 1)]
    pltpu.make_async_copy(part, part, gram_send).wait()


def write_kernel(fresh, held, new_weights, new_momentum, sems):
    pieces = 4
    size = fresh.shape[0] // pieces
    copies = [
        pltpu.make_async_copy(a.at[pl.ds(i * size, size)], b.at[pl.ds(i * size, size)], sems.at[k, i])
        for k, (a, b) in enumerate(((held, new_momentum), (fresh, new_weights)))
        for i in range(pieces)
    ]
    for copy in copies:
        copy.start()
    for copy in copies:
        copy.wait()


def solution(mesh):
    shards, models = mesh.shape["shard"], mesh.shape["model"]

    def folded(x):
        mats, two, wide = x.shape
        x = x.reshape(mats, two, wide // LANES, LANES).transpose(0, 2, 1, 3)
        return x.reshape(shards, mats // (shards * PAIR), ROWS, LANES)

    def unfolded(x, like):
        mats, two, wide = like.shape
        x = x.reshape(mats, wide // LANES, two, LANES).transpose(0, 2, 1, 3)
        return x.reshape(like.shape)

    def on_device(grad_stack, moment_stack, weight_stack):
        grad, moment, weight = folded(grad_stack), folded(moment_stack), folded(weight_stack)
        shape = grad.shape
        chunks = shape[1]
        side, wide = 2 * shards, TILE // 2 * LANES
        vmem = pl.BlockSpec(memory_space=pltpu.VMEM)
        far = pl.BlockSpec(memory_space=pltpu.HBM)
        block = jax.ShapeDtypeStruct(shape, F32)
        fresh, held = pl.pallas_call(
            functools.partial(exchange_kernel, shards, models, chunks),
            name="exchange",
            out_shape=(block, block),
            in_specs=[far, far, far],
            out_specs=(vmem, vmem),
            scratch_shapes=[
                pltpu.VMEM(shape, F32),
                pltpu.VMEM(shape, F32),
                pltpu.VMEM(shape, F32),
                pltpu.VMEM((chunks, shards * ROWS, LANES), F32),
                pltpu.VMEM((chunks, PAIR, side, wide), F32),
                pltpu.VMEM((chunks, PAIR, side, wide), F32),
                pltpu.VMEM((chunks, shards * ROWS, LANES), F32),
                pltpu.VMEM((chunks, shards * ROWS, LANES), F32),
                pltpu.VMEM((2, chunks, models, PAIR, side, side), F32),
                pltpu.SemaphoreType.DMA((3, chunks)),
                pltpu.SemaphoreType.DMA,
                pltpu.SemaphoreType.DMA((chunks,)),
                pltpu.SemaphoreType.DMA,
                pltpu.SemaphoreType.DMA((2, chunks)),
                pltpu.SemaphoreType.DMA,
                pltpu.SemaphoreType.DMA((chunks,)),
            ],
            compiler_params=pltpu.CompilerParams(
                collective_id=0, has_side_effects=True, vmem_limit_bytes=48 * 1024 * 1024
            ),
        )(grad, moment, weight)
        new_weights, new_momentum = pl.pallas_call(
            write_kernel,
            name="write",
            out_shape=(block, block),
            in_specs=[vmem, vmem],
            out_specs=(far, far),
            scratch_shapes=[pltpu.SemaphoreType.DMA((2, 4))],
            compiler_params=pltpu.CompilerParams(vmem_limit_bytes=16 * 1024 * 1024),
        )(fresh, held)
        return unfolded(new_weights, weight_stack), unfolded(new_momentum, weight_stack)

    spec = P(None, "shard", "model")
    return jax.shard_map(on_device, mesh=mesh, in_specs=(spec,) * 3, out_specs=(spec,) * 2, check_vma=False)
```

```python
import functools

import jax
import jax.numpy as jnp
from jax import lax
from jax.experimental import pallas as pl
from jax.experimental.pallas import tpu as pltpu
from jax.sharding import PartitionSpec as P

hold_rate = 0.95
learn_rate = 1.0
decay_rate = 0.1
HIGH = lax.Precision.HIGHEST
MESH = pl.DeviceIdType.MESH
F32 = jnp.float32

LANES = 128
TILE = 8
PAIR = 1
ROWS = PAIR * TILE


def mul(a, b):
    return lax.dot_general(a, b, (((1,), (0,)), ((), ())), precision=HIGH, preferred_element_type=F32)


def gram_of(x):
    return lax.dot_general(x, x, (((1,), (1,)), ((), ())), precision=HIGH, preferred_element_type=F32)


def diagonal(side):
    return lax.broadcasted_iota(jnp.int32, (side, side), 0) == lax.broadcasted_iota(jnp.int32, (side, side), 1)


def chain(grams, steps):
    eye = jnp.where(diagonal(grams[0].shape[0]), 3.4445, 0.0).astype(F32)
    totals = None
    for step in range(steps):
        squares = [mul(a, a) for a in grams]
        factors = [eye - 4.775 * a + 2.0315 * s for a, s in zip(grams, squares)]
        totals = factors if totals is None else [mul(f, t) for f, t in zip(factors, totals)]
        if step < steps - 1:
            half = [mul(f, a) for f, a in zip(factors, grams)]
            grams = [mul(h, f) for h, f in zip(half, factors)]
    return totals


def peers_in_order(me, shards):
    depth, flat = shards // 8, 8
    z, rest = me // flat, lax.rem(me, flat)
    x, core = rest // 2, lax.rem(rest, 2)
    around = [0] + [d for k in range(1, depth) for d in (k, depth - k)][: depth - 1]
    around = around[1:] + around[:1]
    zs = [lax.rem(z + d, depth) * flat for d in around]
    xs = [lax.rem(x + dx, 4) * 2 + lax.rem(core + dc, 2) for dx in (0, 1, 3, 2) for dc in (0, 1)]
    order = [(zs[(i + j) % depth], xs[j], around[(i + j) % depth], j) for i in range(depth) for j in range(flat)]
    return [a + b for a, b, d, j in order if (d, j) != (0, 0)]


def exchange_kernel(
    shards, models, chunks,
    grad, moment, weight, fresh, held,
    grad_in, moment_in, weight_in, rows, whole, moved, out, back, grams,
    in_sem, go_send, go_recv, gram_send, gram_recv, home_send, home_recv,
):
    me, mine = lax.axis_index("shard"), lax.axis_index("model")
    side = 2 * shards
    barrier = pltpu.get_barrier_semaphore()
    peers = peers_in_order(me, shards)
    others = [lax.rem(mine + step, models) for step in range(1, models)]

    for peer in peers:
        pl.semaphore_signal(barrier, inc=1, device_id=(peer, mine), device_id_type=MESH)
    for other in others:
        pl.semaphore_signal(barrier, inc=1, device_id=(me, other), device_id_type=MESH)

    def load(source, target, which, chunk):
        return pltpu.make_async_copy(source.at[:, chunk], target.at[:, chunk], in_sem.at[which, chunk])

    for chunk in range(chunks):
        load(grad, grad_in, 0, chunk).start()
        load(moment, moment_in, 1, chunk).start()
    for chunk in range(chunks):
        load(grad, grad_in, 0, chunk).wait()
        load(moment, moment_in, 1, chunk).wait()
        held[:, chunk] = hold_rate * moment_in[:, chunk] + grad_in[:, chunk]

    pl.semaphore_wait(barrier, len(peers) + len(others))

    def slot(peer):
        return pl.ds(pl.multiple_of(peer * ROWS, ROWS), ROWS)

    @pl.loop(0, chunks)
    def _(chunk):
        for peer in peers:
            pltpu.make_async_remote_copy(
                src_ref=held.at[peer, chunk], dst_ref=rows.at[chunk, slot(me)],
                send_sem=go_send, recv_sem=go_recv.at[chunk],
                device_id=(peer, mine), device_id_type=MESH,
            ).start()
        rows[chunk, slot(me)] = held[me, chunk]

    for chunk in range(chunks):
        load(weight, weight_in, 2, chunk).start()

    def landed(chunk):
        return rows.at[chunk, pl.ds(0, (shards - 1) * ROWS)]

    def share_gram(turn, chunk):
        for other in others:
            pltpu.make_async_remote_copy(
                src_ref=grams.at[turn, chunk, mine], dst_ref=grams.at[turn, chunk, mine],
                send_sem=gram_send, recv_sem=gram_recv.at[turn, chunk],
                device_id=(me, other), device_id_type=MESH,
            ).start()

    def summed_grams(turn, chunk):
        part = grams.at[turn, chunk, pl.ds(0, models - 1)]
        pltpu.make_async_copy(part, part, gram_recv.at[turn, chunk]).wait()
        sums = []
        for i in range(PAIR):
            total = grams[turn, chunk, 0, i]
            for k in range(1, models):
                total = total + grams[turn, chunk, k, i]
            sums.append(total)
        return sums

    def first_stage(chunk):
        part = landed(chunk)
        pltpu.make_async_copy(part, part, go_recv.at[chunk]).wait()
        for i in range(PAIR):
            for c in range(TILE // 2):
                for r in range(2):
                    whole[chunk, i, pl.ds(r * shards, shards), pl.ds(c * LANES, LANES)] = rows[
                        chunk, pl.ds(i * TILE + 2 * c + r, shards, stride=ROWS), :
                    ]
        for i in range(PAIR):
            grams[0, chunk, mine, i] = gram_of(whole[chunk, i])
        share_gram(0, chunk)

    def second_stage(chunk):
        sums = summed_grams(0, chunk)
        mask = diagonal(side)
        scales = [
            lax.rsqrt(jnp.sum(jnp.sum(jnp.where(mask, g, 0.0), axis=1, keepdims=True), axis=0, keepdims=True) + 1e-06)
            for g in sums
        ]
        factors = chain([g * s * s for g, s in zip(sums, scales)], 2)
        for i in range(PAIR):
            moved[chunk, i] = mul(factors[i] * scales[i], whole[chunk, i])
        for i in range(PAIR):
            grams[1, chunk, mine, i] = gram_of(moved[chunk, i])
        share_gram(1, chunk)

    def third_stage(chunk):
        factors = chain(summed_grams(1, chunk), 3)
        for i in range(PAIR):
            final = mul(factors[i], moved[chunk, i])
            for c in range(TILE // 2):
                for r in range(2):
                    out[chunk, pl.ds(i * TILE + 2 * c + r, shards, stride=ROWS), :] = final[
                        r * shards : (r + 1) * shards, c * LANES : (c + 1) * LANES
                    ]

        for peer in peers:
            pltpu.make_async_remote_copy(
                src_ref=out.at[chunk, slot(peer)], dst_ref=back.at[chunk, slot(me)],
                send_sem=home_send, recv_sem=home_recv.at[chunk],
                device_id=(peer, mine), device_id_type=MESH,
            ).start()
        back[chunk, slot(me)] = out[chunk, slot(me)]

    @pl.loop(0, chunks + 2)
    def _(turn):
        @pl.when(turn < chunks)
        def _():
            first_stage(turn)

        @pl.when((turn >= 1) & (turn <= chunks))
        def _():
            second_stage(turn - 1)

        @pl.when(turn >= 2)
        def _():
            third_stage(turn - 2)

    for chunk in range(chunks):
        load(weight, weight_in, 2, chunk).wait()
        part = back.at[chunk, pl.ds(0, (shards - 1) * ROWS)]
        pltpu.make_async_copy(part, part, home_recv.at[chunk]).wait()
        fresh[:, chunk] = (1.0 - learn_rate * decay_rate) * weight_in[:, chunk] - learn_rate * back[chunk].reshape(
            shards, ROWS, LANES
        )

    part = held.at[pl.ds(0, shards - 1)]
    pltpu.make_async_copy(part, part, home_send).wait()
    pltpu.make_async_copy(part, part, go_send).wait()
    part = grams.at[:, :, pl.ds(0, models - 1)]
    pltpu.make_async_copy(part, part, gram_send).wait()


def write_kernel(fresh, held, new_weights, new_momentum, sems):
    pieces = 4
    size = fresh.shape[0] // pieces
    copies = [
        pltpu.make_async_copy(a.at[pl.ds(i * size, size)], b.at[pl.ds(i * size, size)], sems.at[k, i])
        for k, (a, b) in enumerate(((held, new_momentum), (fresh, new_weights)))
        for i in range(pieces)
    ]
    for copy in copies:
        copy.start()
    for copy in copies:
        copy.wait()


def solution(mesh):
    shards, models = mesh.shape["shard"], mesh.shape["model"]

    def folded(x):
        mats, two, wide = x.shape
        x = x.reshape(mats, two, wide // LANES, LANES).transpose(0, 2, 1, 3)
        return x.reshape(shards, mats // (shards * PAIR), ROWS, LANES)

    def unfolded(x, like):
        mats, two, wide = like.shape
        x = x.reshape(mats, wide // LANES, two, LANES).transpose(0, 2, 1, 3)
        return x.reshape(like.shape)

    def on_device(grad_stack, moment_stack, weight_stack):
        grad, moment, weight = folded(grad_stack), folded(moment_stack), folded(weight_stack)
        shape = grad.shape
        chunks = shape[1]
        side, wide = 2 * shards, TILE // 2 * LANES
        vmem = pl.BlockSpec(memory_space=pltpu.VMEM)
        far = pl.BlockSpec(memory_space=pltpu.HBM)
        block = jax.ShapeDtypeStruct(shape, F32)
        fresh, held = pl.pallas_call(
            functools.partial(exchange_kernel, shards, models, chunks),
            name="exchange",
            out_shape=(block, block),
            in_specs=[far, far, far],
            out_specs=(vmem, vmem),
            scratch_shapes=[
                pltpu.VMEM(shape, F32),
                pltpu.VMEM(shape, F32),
                pltpu.VMEM(shape, F32),
                pltpu.VMEM((chunks, shards * ROWS, LANES), F32),
                pltpu.VMEM((chunks, PAIR, side, wide), F32),
                pltpu.VMEM((chunks, PAIR, side, wide), F32),
                pltpu.VMEM((chunks, shards * ROWS, LANES), F32),
                pltpu.VMEM((chunks, shards * ROWS, LANES), F32),
                pltpu.VMEM((2, chunks, models, PAIR, side, side), F32),
                pltpu.SemaphoreType.DMA((3, chunks)),
                pltpu.SemaphoreType.DMA,
                pltpu.SemaphoreType.DMA((chunks,)),
                pltpu.SemaphoreType.DMA,
                pltpu.SemaphoreType.DMA((2, chunks)),
                pltpu.SemaphoreType.DMA,
                pltpu.SemaphoreType.DMA((chunks,)),
            ],
            compiler_params=pltpu.CompilerParams(
                collective_id=0, has_side_effects=True, vmem_limit_bytes=48 * 1024 * 1024
            ),
        )(grad, moment, weight)
        new_weights, new_momentum = pl.pallas_call(
            write_kernel,
            name="write",
            out_shape=(block, block),
            in_specs=[vmem, vmem],
            out_specs=(far, far),
            scratch_shapes=[pltpu.SemaphoreType.DMA((2, 4))],
            compiler_params=pltpu.CompilerParams(vmem_limit_bytes=16 * 1024 * 1024),
        )(fresh, held)
        return unfolded(new_weights, weight_stack), unfolded(new_momentum, weight_stack)

    spec = P(None, "shard", "model")
    return jax.shard_map(on_device, mesh=mesh, in_specs=(spec,) * 3, out_specs=(spec,) * 2, check_vma=False)
```

```python
import functools

import jax
import jax.numpy as jnp
from jax import lax
from jax.experimental import pallas as pl
from jax.experimental.pallas import tpu as pltpu
from jax.sharding import PartitionSpec as P

hold_rate = 0.95
learn_rate = 1.0
decay_rate = 0.1
HIGH = lax.Precision.HIGHEST
MESH = pl.DeviceIdType.MESH
F32 = jnp.float32

LANES = 128
TILE = 8
PAIR = 1
ROWS = PAIR * TILE


def mul(a, b):
    return lax.dot_general(a, b, (((1,), (0,)), ((), ())), precision=HIGH, preferred_element_type=F32)


def gram_of(x):
    return lax.dot_general(x, x, (((1,), (1,)), ((), ())), precision=HIGH, preferred_element_type=F32)


def diagonal(side):
    return lax.broadcasted_iota(jnp.int32, (side, side), 0) == lax.broadcasted_iota(jnp.int32, (side, side), 1)


def chain(grams, steps):
    eye = jnp.where(diagonal(grams[0].shape[0]), 3.4445, 0.0).astype(F32)
    totals = None
    for step in range(steps):
        squares = [mul(a, a) for a in grams]
        factors = [eye - 4.775 * a + 2.0315 * s for a, s in zip(grams, squares)]
        totals = factors if totals is None else [mul(f, t) for f, t in zip(factors, totals)]
        if step < steps - 1:
            half = [mul(f, a) for f, a in zip(factors, grams)]
            grams = [mul(h, f) for h, f in zip(half, factors)]
    return totals


def around(size):
    return [d for k in range(1, size) for d in (k, size - k)][: size - 1]


def exchange_kernel(
    shards, models, chunks,
    grad, moment, weight, fresh, held,
    grad_in, moment_in, weight_in, came, rows, whole, moved, out, left, back, grams,
    in_sem, go_far_send, go_far_recv, go_near_send, go_near_recv, gram_send, gram_recv,
    home_near_send, home_near_recv, home_far_send, home_far_recv,
):
    me, mine = lax.axis_index("shard"), lax.axis_index("model")
    side = 2 * shards
    barrier = pltpu.get_barrier_semaphore()
    near_size = came.shape[1]
    far_size = shards // near_size
    far, near = me // near_size, lax.rem(me, near_size)
    x, core = near // 2, lax.rem(near, 2)
    fars = [lax.rem(far + d, far_size) for d in around(far_size)]
    nears = [
        lax.rem(x + dx, near_size // 2) * 2 + lax.rem(core + dc, 2)
        for dx in [*around(near_size // 2), 0]
        for dc in (0, 1)
        if dx + dc > 0
    ]
    others = [lax.rem(mine + step, models) for step in range(1, models)]

    for peer in fars:
        pl.semaphore_signal(barrier, inc=1, device_id=(peer * near_size + near, mine), device_id_type=MESH)
    for peer in nears:
        pl.semaphore_signal(barrier, inc=1, device_id=(far * near_size + peer, mine), device_id_type=MESH)
    for other in others:
        pl.semaphore_signal(barrier, inc=1, device_id=(me, other), device_id_type=MESH)

    def load(source, target, which, chunk):
        return pltpu.make_async_copy(source.at[:, chunk], target.at[:, chunk], in_sem.at[which, chunk])

    for chunk in range(chunks):
        load(grad, grad_in, 0, chunk).start()
        load(moment, moment_in, 1, chunk).start()

    def ready(chunk):
        load(grad, grad_in, 0, chunk).wait()
        load(moment, moment_in, 1, chunk).wait()
        held[:, chunk] = hold_rate * moment_in[:, chunk] + grad_in[:, chunk]

    ready(0)
    pl.semaphore_wait(barrier, len(fars) + len(nears) + len(others))

    def group(peer):
        size = far_size * ROWS
        return pl.ds(pl.multiple_of(peer * size, size), size)

    def slot(peer):
        return pl.ds(pl.multiple_of(peer * ROWS, ROWS), ROWS)

    def targets(peer):
        return pl.ds(pl.multiple_of(peer * near_size, near_size), near_size)

    def landed(ref, sem):
        pltpu.make_async_copy(ref, ref, sem).wait()

    for chunk in range(chunks):
        for peer in fars:
            pltpu.make_async_remote_copy(
                src_ref=held.at[targets(peer), chunk], dst_ref=came.at[chunk, :, slot(far)],
                send_sem=go_far_send, recv_sem=go_far_recv.at[chunk],
                device_id=(peer * near_size + near, mine), device_id_type=MESH,
            ).start()
        if chunk + 1 < chunks:
            ready(chunk + 1)

    @pl.loop(0, chunks)
    def _(chunk):
        came[chunk, :, slot(far)] = held[targets(far), chunk]

    for chunk in range(chunks):
        load(weight, weight_in, 2, chunk).start()

    def relay_out(chunk):
        landed(came.at[chunk, :, pl.ds(0, (far_size - 1) * ROWS)], go_far_recv.at[chunk])
        for peer in nears:
            pltpu.make_async_remote_copy(
                src_ref=came.at[chunk, peer], dst_ref=rows.at[chunk, group(near)],
                send_sem=go_near_send, recv_sem=go_near_recv.at[chunk],
                device_id=(far * near_size + peer, mine), device_id_type=MESH,
            ).start()
        rows[chunk, group(near)] = came[chunk, near]

    def share_gram(turn, chunk):
        for other in others:
            pltpu.make_async_remote_copy(
                src_ref=grams.at[turn, chunk, mine], dst_ref=grams.at[turn, chunk, mine],
                send_sem=gram_send, recv_sem=gram_recv.at[turn, chunk],
                device_id=(me, other), device_id_type=MESH,
            ).start()

    def summed_grams(turn, chunk):
        landed(grams.at[turn, chunk, pl.ds(0, models - 1)], gram_recv.at[turn, chunk])
        sums = []
        for i in range(PAIR):
            total = grams[turn, chunk, 0, i]
            for k in range(1, models):
                total = total + grams[turn, chunk, k, i]
            sums.append(total)
        return sums

    def first_stage(chunk):
        landed(rows.at[chunk, pl.ds(0, (near_size - 1) * far_size * ROWS)], go_near_recv.at[chunk])
        for i in range(PAIR):
            for c in range(TILE // 2):
                for r in range(2):
                    whole[chunk, i, pl.ds(r * shards, shards), pl.ds(c * LANES, LANES)] = rows[
                        chunk, pl.ds(i * TILE + 2 * c + r, shards, stride=ROWS), :
                    ]
        for i in range(PAIR):
            grams[0, chunk, mine, i] = gram_of(whole[chunk, i])
        share_gram(0, chunk)

    def second_stage(chunk):
        sums = summed_grams(0, chunk)
        mask = diagonal(side)
        scales = [
            lax.rsqrt(jnp.sum(jnp.sum(jnp.where(mask, g, 0.0), axis=1, keepdims=True), axis=0, keepdims=True) + 1e-06)
            for g in sums
        ]
        factors = chain([g * s * s for g, s in zip(sums, scales)], 2)
        for i in range(PAIR):
            moved[chunk, i] = mul(factors[i] * scales[i], whole[chunk, i])
        for i in range(PAIR):
            grams[1, chunk, mine, i] = gram_of(moved[chunk, i])
        share_gram(1, chunk)

    def third_stage(chunk):
        factors = chain(summed_grams(1, chunk), 3)
        for i in range(PAIR):
            final = mul(factors[i], moved[chunk, i])
            for c in range(TILE // 2):
                for r in range(2):
                    out[chunk, pl.ds(i * TILE + 2 * c + r, shards, stride=ROWS), :] = final[
                        r * shards : (r + 1) * shards, c * LANES : (c + 1) * LANES
                    ]

        left[chunk, near] = out[chunk, group(near)]
        for peer in nears:
            pltpu.make_async_remote_copy(
                src_ref=out.at[chunk, group(peer)], dst_ref=left.at[chunk, near],
                send_sem=home_near_send, recv_sem=home_near_recv.at[chunk],
                device_id=(far * near_size + peer, mine), device_id_type=MESH,
            ).start()

    def relay_home(chunk):
        landed(left.at[chunk, pl.ds(0, near_size - 1)], home_near_recv.at[chunk])
        for peer in fars:
            pltpu.make_async_remote_copy(
                src_ref=left.at[chunk, :, slot(peer)], dst_ref=back.at[chunk, far],
                send_sem=home_far_send, recv_sem=home_far_recv.at[chunk],
                device_id=(peer * near_size + near, mine), device_id_type=MESH,
            ).start()
        back[chunk, far] = left[chunk, :, slot(far)]

    stages = (relay_out, first_stage, second_stage, third_stage, relay_home)
    delays = (0, 1, 2, 3, 4)

    @pl.loop(0, chunks + delays[-1])
    def _(turn):
        for late, stage in zip(delays, stages):

            @pl.when((turn >= late) & (turn < chunks + late))
            def _():
                stage(turn - late)

    for chunk in range(chunks):
        load(weight, weight_in, 2, chunk).wait()
        landed(back.at[chunk, pl.ds(0, far_size - 1)], home_far_recv.at[chunk])
        fresh[:, chunk] = (1.0 - learn_rate * decay_rate) * weight_in[:, chunk] - learn_rate * back[chunk].reshape(
            shards, ROWS, LANES
        )

    for sem in (go_far_send, home_far_send):
        landed(came.at[:, :, pl.ds(0, (far_size - 1) * ROWS)], sem)
    for sem in (go_near_send, home_near_send):
        landed(came.at[:, pl.ds(0, near_size - 1)], sem)
    landed(grams.at[:, :, pl.ds(0, models - 1)], gram_send)


def write_kernel(fresh, held, new_weights, new_momentum, sems):
    pieces = 4
    size = fresh.shape[0] // pieces
    copies = [
        pltpu.make_async_copy(a.at[pl.ds(i * size, size)], b.at[pl.ds(i * size, size)], sems.at[k, i])
        for k, (a, b) in enumerate(((held, new_momentum), (fresh, new_weights)))
        for i in range(pieces)
    ]
    for copy in copies:
        copy.start()
    for copy in copies:
        copy.wait()


def solution(mesh):
    shards, models = mesh.shape["shard"], mesh.shape["model"]

    def folded(x):
        mats, two, wide = x.shape
        x = x.reshape(mats, two, wide // LANES, LANES).transpose(0, 2, 1, 3)
        return x.reshape(shards, mats // (shards * PAIR), ROWS, LANES)

    def unfolded(x, like):
        mats, two, wide = like.shape
        x = x.reshape(mats, wide // LANES, two, LANES).transpose(0, 2, 1, 3)
        return x.reshape(like.shape)

    def on_device(grad_stack, moment_stack, weight_stack):
        grad, moment, weight = folded(grad_stack), folded(moment_stack), folded(weight_stack)
        shape = grad.shape
        chunks = shape[1]
        side, wide = 2 * shards, TILE // 2 * LANES
        near, far = 8, shards // 8
        vmem = pl.BlockSpec(memory_space=pltpu.VMEM)
        hbm = pl.BlockSpec(memory_space=pltpu.HBM)
        block = jax.ShapeDtypeStruct(shape, F32)
        fresh, held = pl.pallas_call(
            functools.partial(exchange_kernel, shards, models, chunks),
            name="exchange",
            out_shape=(block, block),
            in_specs=[hbm, hbm, hbm],
            out_specs=(vmem, vmem),
            scratch_shapes=[
                pltpu.VMEM(shape, F32),
                pltpu.VMEM(shape, F32),
                pltpu.VMEM(shape, F32),
                pltpu.VMEM((chunks, near, far * ROWS, LANES), F32),
                pltpu.VMEM((chunks, shards * ROWS, LANES), F32),
                pltpu.VMEM((chunks, PAIR, side, wide), F32),
                pltpu.VMEM((chunks, PAIR, side, wide), F32),
                pltpu.VMEM((chunks, shards * ROWS, LANES), F32),
                pltpu.VMEM((chunks, near, far * ROWS, LANES), F32),
                pltpu.VMEM((chunks, far, near, ROWS, LANES), F32),
                pltpu.VMEM((2, chunks, models, PAIR, side, side), F32),
                pltpu.SemaphoreType.DMA((3, chunks)),
                pltpu.SemaphoreType.DMA,
                pltpu.SemaphoreType.DMA((chunks,)),
                pltpu.SemaphoreType.DMA,
                pltpu.SemaphoreType.DMA((chunks,)),
                pltpu.SemaphoreType.DMA,
                pltpu.SemaphoreType.DMA((2, chunks)),
                pltpu.SemaphoreType.DMA,
                pltpu.SemaphoreType.DMA((chunks,)),
                pltpu.SemaphoreType.DMA,
                pltpu.SemaphoreType.DMA((chunks,)),
            ],
            compiler_params=pltpu.CompilerParams(
                collective_id=0, has_side_effects=True, vmem_limit_bytes=48 * 1024 * 1024
            ),
        )(grad, moment, weight)
        new_weights, new_momentum = pl.pallas_call(
            write_kernel,
            name="write",
            out_shape=(block, block),
            in_specs=[vmem, vmem],
            out_specs=(hbm, hbm),
            scratch_shapes=[pltpu.SemaphoreType.DMA((2, 4))],
            compiler_params=pltpu.CompilerParams(vmem_limit_bytes=16 * 1024 * 1024),
        )(fresh, held)
        return unfolded(new_weights, weight_stack), unfolded(new_momentum, weight_stack)

    spec = P(None, "shard", "model")
    return jax.shard_map(on_device, mesh=mesh, in_specs=(spec,) * 3, out_specs=(spec,) * 2, check_vma=False)
```

```python
import functools

import jax
import jax.numpy as jnp
from jax import lax
from jax.experimental import pallas as pl
from jax.experimental.pallas import tpu as pltpu
from jax.sharding import PartitionSpec as P

hold_rate = 0.95
learn_rate = 1.0
decay_rate = 0.1
HIGH = lax.Precision.HIGHEST
MESH = pl.DeviceIdType.MESH
F32 = jnp.float32

LANES = 128
TILE = 8
PAIR = 1
ROWS = PAIR * TILE


def mul(a, b):
    return lax.dot_general(a, b, (((1,), (0,)), ((), ())), precision=HIGH, preferred_element_type=F32)


def gram_of(x):
    return lax.dot_general(x, x, (((1,), (1,)), ((), ())), precision=HIGH, preferred_element_type=F32)


def diagonal(side):
    return lax.broadcasted_iota(jnp.int32, (side, side), 0) == lax.broadcasted_iota(jnp.int32, (side, side), 1)


def chain(grams, steps):
    eye = jnp.where(diagonal(grams[0].shape[0]), 3.4445, 0.0).astype(F32)
    totals = None
    for step in range(steps):
        squares = [mul(a, a) for a in grams]
        factors = [eye - 4.775 * a + 2.0315 * s for a, s in zip(grams, squares)]
        totals = factors if totals is None else [mul(f, t) for f, t in zip(factors, totals)]
        if step < steps - 1:
            half = [mul(f, a) for f, a in zip(factors, grams)]
            grams = [mul(h, f) for h, f in zip(half, factors)]
    return totals


def around(size):
    return [d for k in range(1, size) for d in (k, size - k)][: size - 1]


def exchange_kernel(
    shards, models, chunks,
    grad, moment, weight, fresh, held,
    grad_in, moment_in, weight_in, came, rows, whole, moved, out, left, back, grams,
    in_sem, go_far_send, go_far_recv, go_near_send, go_near_recv, gram_send, gram_recv,
    home_near_send, home_near_recv, home_far_send, home_far_recv,
):
    me, mine = lax.axis_index("shard"), lax.axis_index("model")
    side = 2 * shards
    barrier = pltpu.get_barrier_semaphore()
    near_size = came.shape[1]
    far_size = shards // near_size
    far, near = me // near_size, lax.rem(me, near_size)
    x, core = near // 2, lax.rem(near, 2)
    fars = [lax.rem(far + d, far_size) for d in around(far_size)]
    nears = [
        lax.rem(x + dx, near_size // 2) * 2 + lax.rem(core + dc, 2)
        for dx in [*around(near_size // 2), 0]
        for dc in (0, 1)
        if dx + dc > 0
    ]
    others = [lax.rem(mine + step, models) for step in range(1, models)]

    for peer in fars:
        pl.semaphore_signal(barrier, inc=1, device_id=(peer * near_size + near, mine), device_id_type=MESH)
    for peer in nears:
        pl.semaphore_signal(barrier, inc=1, device_id=(far * near_size + peer, mine), device_id_type=MESH)
    for other in others:
        pl.semaphore_signal(barrier, inc=1, device_id=(me, other), device_id_type=MESH)

    def load(source, target, which, chunk):
        return pltpu.make_async_copy(source.at[:, chunk], target.at[:, chunk], in_sem.at[which, chunk])

    for chunk in range(chunks):
        load(grad, grad_in, 0, chunk).start()
        load(moment, moment_in, 1, chunk).start()

    def ready(chunk):
        load(grad, grad_in, 0, chunk).wait()
        load(moment, moment_in, 1, chunk).wait()
        held[:, chunk] = hold_rate * moment_in[:, chunk] + grad_in[:, chunk]

    ready(0)
    pl.semaphore_wait(barrier, len(fars) + len(nears) + len(others))

    def group(peer):
        size = far_size * ROWS
        return pl.ds(pl.multiple_of(peer * size, size), size)

    def slot(peer):
        return pl.ds(pl.multiple_of(peer * ROWS, ROWS), ROWS)

    def targets(peer):
        return pl.ds(pl.multiple_of(peer * near_size, near_size), near_size)

    def landed(ref, sem):
        pltpu.make_async_copy(ref, ref, sem).wait()

    for chunk in range(chunks):
        for peer in fars:
            pltpu.make_async_remote_copy(
                src_ref=held.at[targets(peer), chunk], dst_ref=came.at[chunk, :, slot(far)],
                send_sem=go_far_send, recv_sem=go_far_recv.at[chunk],
                device_id=(peer * near_size + near, mine), device_id_type=MESH,
            ).start()
        if chunk + 1 < chunks:
            ready(chunk + 1)

    @pl.loop(0, chunks)
    def _(chunk):
        came[chunk, :, slot(far)] = held[targets(far), chunk]

    for chunk in range(chunks):
        load(weight, weight_in, 2, chunk).start()

    def relay_out(chunk):
        landed(came.at[chunk, :, pl.ds(0, (far_size - 1) * ROWS)], go_far_recv.at[chunk])
        for peer in nears:
            pltpu.make_async_remote_copy(
                src_ref=came.at[chunk, peer], dst_ref=rows.at[chunk, group(near)],
                send_sem=go_near_send, recv_sem=go_near_recv.at[chunk],
                device_id=(far * near_size + peer, mine), device_id_type=MESH,
            ).start()
        rows[chunk, group(near)] = came[chunk, near]

    def share_gram(turn, chunk):
        for other in others:
            pltpu.make_async_remote_copy(
                src_ref=grams.at[turn, chunk, mine], dst_ref=grams.at[turn, chunk, mine],
                send_sem=gram_send, recv_sem=gram_recv.at[turn, chunk],
                device_id=(me, other), device_id_type=MESH,
            ).start()

    def summed_grams(turn, chunk):
        landed(grams.at[turn, chunk, pl.ds(0, models - 1)], gram_recv.at[turn, chunk])
        sums = []
        for i in range(PAIR):
            total = grams[turn, chunk, 0, i]
            for k in range(1, models):
                total = total + grams[turn, chunk, k, i]
            sums.append(total)
        return sums

    def first_stage(chunk):
        landed(rows.at[chunk, pl.ds(0, (near_size - 1) * far_size * ROWS)], go_near_recv.at[chunk])
        for i in range(PAIR):
            for c in range(TILE // 2):
                for r in range(2):
                    whole[chunk, i, pl.ds(r * shards, shards), pl.ds(c * LANES, LANES)] = rows[
                        chunk, pl.ds(i * TILE + 2 * c + r, shards, stride=ROWS), :
                    ]
        for i in range(PAIR):
            grams[0, chunk, mine, i] = gram_of(whole[chunk, i])
        share_gram(0, chunk)

    def second_stage(chunk):
        sums = summed_grams(0, chunk)
        mask = diagonal(side)
        scales = [
            lax.rsqrt(jnp.sum(jnp.sum(jnp.where(mask, g, 0.0), axis=1, keepdims=True), axis=0, keepdims=True) + 1e-06)
            for g in sums
        ]
        factors = chain([g * s * s for g, s in zip(sums, scales)], 2)
        for i in range(PAIR):
            moved[chunk, i] = mul(factors[i] * scales[i], whole[chunk, i])
        for i in range(PAIR):
            grams[1, chunk, mine, i] = gram_of(moved[chunk, i])
        share_gram(1, chunk)

    def third_stage(chunk):
        factors = chain(summed_grams(1, chunk), 3)
        for i in range(PAIR):
            final = mul(factors[i], moved[chunk, i])
            for c in range(TILE // 2):
                for r in range(2):
                    out[chunk, pl.ds(i * TILE + 2 * c + r, shards, stride=ROWS), :] = final[
                        r * shards : (r + 1) * shards, c * LANES : (c + 1) * LANES
                    ]

        left[chunk, near] = out[chunk, group(near)]
        for peer in nears:
            pltpu.make_async_remote_copy(
                src_ref=out.at[chunk, group(peer)], dst_ref=left.at[chunk, near],
                send_sem=home_near_send, recv_sem=home_near_recv.at[chunk],
                device_id=(far * near_size + peer, mine), device_id_type=MESH,
            ).start()

    def relay_home(chunk):
        landed(left.at[chunk, pl.ds(0, near_size - 1)], home_near_recv.at[chunk])
        for peer in reversed(fars):
            pltpu.make_async_remote_copy(
                src_ref=left.at[chunk, :, slot(peer)], dst_ref=back.at[chunk, far],
                send_sem=home_far_send, recv_sem=home_far_recv.at[chunk],
                device_id=(peer * near_size + near, mine), device_id_type=MESH,
            ).start()
        back[chunk, far] = left[chunk, :, slot(far)]

    stages = (relay_out, first_stage, second_stage, third_stage, relay_home)
    delays = (0, 1, 2, 3, 4)

    @pl.loop(0, chunks + delays[-1])
    def _(turn):
        for late, stage in zip(delays, stages):

            @pl.when((turn >= late) & (turn < chunks + late))
            def _():
                stage(turn - late)

    for chunk in range(chunks):
        load(weight, weight_in, 2, chunk).wait()
        landed(back.at[chunk, pl.ds(0, far_size - 1)], home_far_recv.at[chunk])
        fresh[:, chunk] = (1.0 - learn_rate * decay_rate) * weight_in[:, chunk] - learn_rate * back[chunk].reshape(
            shards, ROWS, LANES
        )

    for sem in (go_far_send, home_far_send):
        landed(came.at[:, :, pl.ds(0, (far_size - 1) * ROWS)], sem)
    for sem in (go_near_send, home_near_send):
        landed(came.at[:, pl.ds(0, near_size - 1)], sem)
    landed(grams.at[:, :, pl.ds(0, models - 1)], gram_send)


def write_kernel(fresh, held, new_weights, new_momentum, sems):
    pieces = 4
    size = fresh.shape[0] // pieces
    copies = [
        pltpu.make_async_copy(a.at[pl.ds(i * size, size)], b.at[pl.ds(i * size, size)], sems.at[k, i])
        for k, (a, b) in enumerate(((held, new_momentum), (fresh, new_weights)))
        for i in range(pieces)
    ]
    for copy in copies:
        copy.start()
    for copy in copies:
        copy.wait()


def solution(mesh):
    shards, models = mesh.shape["shard"], mesh.shape["model"]

    def folded(x):
        mats, two, wide = x.shape
        x = x.reshape(mats, two, wide // LANES, LANES).transpose(0, 2, 1, 3)
        return x.reshape(shards, mats // (shards * PAIR), ROWS, LANES)

    def unfolded(x, like):
        mats, two, wide = like.shape
        x = x.reshape(mats, wide // LANES, two, LANES).transpose(0, 2, 1, 3)
        return x.reshape(like.shape)

    def on_device(grad_stack, moment_stack, weight_stack):
        grad, moment, weight = folded(grad_stack), folded(moment_stack), folded(weight_stack)
        shape = grad.shape
        chunks = shape[1]
        side, wide = 2 * shards, TILE // 2 * LANES
        near, far = 8, shards // 8
        vmem = pl.BlockSpec(memory_space=pltpu.VMEM)
        hbm = pl.BlockSpec(memory_space=pltpu.HBM)
        block = jax.ShapeDtypeStruct(shape, F32)
        fresh, held = pl.pallas_call(
            functools.partial(exchange_kernel, shards, models, chunks),
            name="exchange",
            out_shape=(block, block),
            in_specs=[hbm, hbm, hbm],
            out_specs=(vmem, vmem),
            scratch_shapes=[
                pltpu.VMEM(shape, F32),
                pltpu.VMEM(shape, F32),
                pltpu.VMEM(shape, F32),
                pltpu.VMEM((chunks, near, far * ROWS, LANES), F32),
                pltpu.VMEM((chunks, shards * ROWS, LANES), F32),
                pltpu.VMEM((chunks, PAIR, side, wide), F32),
                pltpu.VMEM((chunks, PAIR, side, wide), F32),
                pltpu.VMEM((chunks, shards * ROWS, LANES), F32),
                pltpu.VMEM((chunks, near, far * ROWS, LANES), F32),
                pltpu.VMEM((chunks, far, near, ROWS, LANES), F32),
                pltpu.VMEM((2, chunks, models, PAIR, side, side), F32),
                pltpu.SemaphoreType.DMA((3, chunks)),
                pltpu.SemaphoreType.DMA,
                pltpu.SemaphoreType.DMA((chunks,)),
                pltpu.SemaphoreType.DMA,
                pltpu.SemaphoreType.DMA((chunks,)),
                pltpu.SemaphoreType.DMA,
                pltpu.SemaphoreType.DMA((2, chunks)),
                pltpu.SemaphoreType.DMA,
                pltpu.SemaphoreType.DMA((chunks,)),
                pltpu.SemaphoreType.DMA,
                pltpu.SemaphoreType.DMA((chunks,)),
            ],
            compiler_params=pltpu.CompilerParams(
                collective_id=0, has_side_effects=True, vmem_limit_bytes=48 * 1024 * 1024
            ),
        )(grad, moment, weight)
        new_weights, new_momentum = pl.pallas_call(
            write_kernel,
            name="write",
            out_shape=(block, block),
            in_specs=[vmem, vmem],
            out_specs=(hbm, hbm),
            scratch_shapes=[pltpu.SemaphoreType.DMA((2, 4))],
            compiler_params=pltpu.CompilerParams(vmem_limit_bytes=16 * 1024 * 1024),
        )(fresh, held)
        return unfolded(new_weights, weight_stack), unfolded(new_momentum, weight_stack)

    spec = P(None, "shard", "model")
    return jax.shard_map(on_device, mesh=mesh, in_specs=(spec,) * 3, out_specs=(spec,) * 2, check_vma=False)
```

```python
import functools

import jax
import jax.numpy as jnp
from jax import lax
from jax.experimental import pallas as pl
from jax.experimental.pallas import tpu as pltpu
from jax.sharding import PartitionSpec as P

hold_rate = 0.95
learn_rate = 1.0
decay_rate = 0.1
HIGH = lax.Precision.HIGHEST
MESH = pl.DeviceIdType.MESH
F32 = jnp.float32

LANES = 128
TILE = 8
PAIR = 1
ROWS = PAIR * TILE


def mul(a, b):
    return lax.dot_general(a, b, (((1,), (0,)), ((), ())), precision=HIGH, preferred_element_type=F32)


def gram_of(x):
    return lax.dot_general(x, x, (((1,), (1,)), ((), ())), precision=HIGH, preferred_element_type=F32)


def diagonal(side):
    return lax.broadcasted_iota(jnp.int32, (side, side), 0) == lax.broadcasted_iota(jnp.int32, (side, side), 1)


def chain(grams, steps):
    eye = jnp.where(diagonal(grams[0].shape[0]), 3.4445, 0.0).astype(F32)
    totals = None
    for step in range(steps):
        squares = [mul(a, a) for a in grams]
        factors = [eye - 4.775 * a + 2.0315 * s for a, s in zip(grams, squares)]
        totals = factors if totals is None else [mul(f, t) for f, t in zip(factors, totals)]
        if step < steps - 1:
            half = [mul(f, a) for f, a in zip(factors, grams)]
            grams = [mul(h, f) for h, f in zip(half, factors)]
    return totals


def around(size):
    return [d for k in range(1, size) for d in (k, size - k)][: size - 1]


def exchange_kernel(
    shards, models, chunks,
    grad, moment, weight, fresh, held,
    grad_in, moment_in, weight_in, came, rows, whole, moved, out, left, back, grams,
    in_sem, go_far_send, go_far_recv, go_near_send, go_near_recv, gram_send, gram_recv,
    home_near_send, home_near_recv, home_far_send, home_far_recv,
):
    me, mine = lax.axis_index("shard"), lax.axis_index("model")
    side = 2 * shards
    barrier = pltpu.get_barrier_semaphore()
    near_size = came.shape[1]
    far_size = shards // near_size
    far, near = me // near_size, lax.rem(me, near_size)
    x, core = near // 2, lax.rem(near, 2)
    fars = [lax.rem(far + d, far_size) for d in around(far_size)]
    nears = [
        lax.rem(x + dx, near_size // 2) * 2 + lax.rem(core + dc, 2)
        for dx in [*reversed(around(near_size // 2)), 0]
        for dc in (0, 1)
        if dx + dc > 0
    ]
    others = [lax.rem(mine + step, models) for step in range(1, models)]

    for peer in fars:
        pl.semaphore_signal(barrier, inc=1, device_id=(peer * near_size + near, mine), device_id_type=MESH)
    for peer in nears:
        pl.semaphore_signal(barrier, inc=1, device_id=(far * near_size + peer, mine), device_id_type=MESH)
    for other in others:
        pl.semaphore_signal(barrier, inc=1, device_id=(me, other), device_id_type=MESH)

    def load(source, target, which, chunk):
        return pltpu.make_async_copy(source.at[:, chunk], target.at[:, chunk], in_sem.at[which, chunk])

    for chunk in range(chunks):
        load(grad, grad_in, 0, chunk).start()
        load(moment, moment_in, 1, chunk).start()

    def ready(chunk):
        load(grad, grad_in, 0, chunk).wait()
        load(moment, moment_in, 1, chunk).wait()
        held[:, chunk] = hold_rate * moment_in[:, chunk] + grad_in[:, chunk]

    ready(0)
    pl.semaphore_wait(barrier, len(fars) + len(nears) + len(others))

    def group(peer):
        size = far_size * ROWS
        return pl.ds(pl.multiple_of(peer * size, size), size)

    def slot(peer):
        return pl.ds(pl.multiple_of(peer * ROWS, ROWS), ROWS)

    def targets(peer):
        return pl.ds(pl.multiple_of(peer * near_size, near_size), near_size)

    def landed(ref, sem):
        pltpu.make_async_copy(ref, ref, sem).wait()

    for chunk in range(chunks):
        for peer in fars:
            pltpu.make_async_remote_copy(
                src_ref=held.at[targets(peer), chunk], dst_ref=came.at[chunk, :, slot(far)],
                send_sem=go_far_send, recv_sem=go_far_recv.at[chunk],
                device_id=(peer * near_size + near, mine), device_id_type=MESH,
            ).start()
        if chunk + 1 < chunks:
            ready(chunk + 1)

    @pl.loop(0, chunks)
    def _(chunk):
        came[chunk, :, slot(far)] = held[targets(far), chunk]

    for chunk in range(chunks):
        load(weight, weight_in, 2, chunk).start()

    def relay_out(chunk):
        landed(came.at[chunk, :, pl.ds(0, (far_size - 1) * ROWS)], go_far_recv.at[chunk])
        for peer in nears:
            pltpu.make_async_remote_copy(
                src_ref=came.at[chunk, peer], dst_ref=rows.at[chunk, group(near)],
                send_sem=go_near_send, recv_sem=go_near_recv.at[chunk],
                device_id=(far * near_size + peer, mine), device_id_type=MESH,
            ).start()
        rows[chunk, group(near)] = came[chunk, near]

    def share_gram(turn, chunk):
        for other in others:
            pltpu.make_async_remote_copy(
                src_ref=grams.at[turn, chunk, mine], dst_ref=grams.at[turn, chunk, mine],
                send_sem=gram_send, recv_sem=gram_recv.at[turn, chunk],
                device_id=(me, other), device_id_type=MESH,
            ).start()

    def summed_grams(turn, chunk):
        landed(grams.at[turn, chunk, pl.ds(0, models - 1)], gram_recv.at[turn, chunk])
        sums = []
        for i in range(PAIR):
            total = grams[turn, chunk, 0, i]
            for k in range(1, models):
                total = total + grams[turn, chunk, k, i]
            sums.append(total)
        return sums

    def first_stage(chunk):
        landed(rows.at[chunk, pl.ds(0, (near_size - 1) * far_size * ROWS)], go_near_recv.at[chunk])
        for i in range(PAIR):
            for c in range(TILE // 2):
                for r in range(2):
                    whole[chunk, i, pl.ds(r * shards, shards), pl.ds(c * LANES, LANES)] = rows[
                        chunk, pl.ds(i * TILE + 2 * c + r, shards, stride=ROWS), :
                    ]
        for i in range(PAIR):
            grams[0, chunk, mine, i] = gram_of(whole[chunk, i])
        share_gram(0, chunk)

    def second_stage(chunk):
        sums = summed_grams(0, chunk)
        mask = diagonal(side)
        scales = [
            lax.rsqrt(jnp.sum(jnp.sum(jnp.where(mask, g, 0.0), axis=1, keepdims=True), axis=0, keepdims=True) + 1e-06)
            for g in sums
        ]
        factors = chain([g * s * s for g, s in zip(sums, scales)], 2)
        for i in range(PAIR):
            moved[chunk, i] = mul(factors[i] * scales[i], whole[chunk, i])
        for i in range(PAIR):
            grams[1, chunk, mine, i] = gram_of(moved[chunk, i])
        share_gram(1, chunk)

    def third_stage(chunk):
        factors = chain(summed_grams(1, chunk), 3)
        for i in range(PAIR):
            final = mul(factors[i], moved[chunk, i])
            for c in range(TILE // 2):
                for r in range(2):
                    out[chunk, pl.ds(i * TILE + 2 * c + r, shards, stride=ROWS), :] = final[
                        r * shards : (r + 1) * shards, c * LANES : (c + 1) * LANES
                    ]

        left[chunk, near] = out[chunk, group(near)]
        for peer in nears:
            pltpu.make_async_remote_copy(
                src_ref=out.at[chunk, group(peer)], dst_ref=left.at[chunk, near],
                send_sem=home_near_send, recv_sem=home_near_recv.at[chunk],
                device_id=(far * near_size + peer, mine), device_id_type=MESH,
            ).start()

    def relay_home(chunk):
        landed(left.at[chunk, pl.ds(0, near_size - 1)], home_near_recv.at[chunk])
        for peer in reversed(fars):
            pltpu.make_async_remote_copy(
                src_ref=left.at[chunk, :, slot(peer)], dst_ref=back.at[chunk, far],
                send_sem=home_far_send, recv_sem=home_far_recv.at[chunk],
                device_id=(peer * near_size + near, mine), device_id_type=MESH,
            ).start()
        back[chunk, far] = left[chunk, :, slot(far)]

    stages = (relay_out, first_stage, second_stage, third_stage, relay_home)
    delays = (0, 1, 2, 3, 4)

    @pl.loop(0, chunks + delays[-1])
    def _(turn):
        for late, stage in zip(delays, stages):

            @pl.when((turn >= late) & (turn < chunks + late))
            def _():
                stage(turn - late)

    for chunk in range(chunks):
        load(weight, weight_in, 2, chunk).wait()
        landed(back.at[chunk, pl.ds(0, far_size - 1)], home_far_recv.at[chunk])
        fresh[:, chunk] = (1.0 - learn_rate * decay_rate) * weight_in[:, chunk] - learn_rate * back[chunk].reshape(
            shards, ROWS, LANES
        )

    for sem in (go_far_send, home_far_send):
        landed(came.at[:, :, pl.ds(0, (far_size - 1) * ROWS)], sem)
    for sem in (go_near_send, home_near_send):
        landed(came.at[:, pl.ds(0, near_size - 1)], sem)
    landed(grams.at[:, :, pl.ds(0, models - 1)], gram_send)


def write_kernel(fresh, held, new_weights, new_momentum, sems):
    pieces = 4
    size = fresh.shape[0] // pieces
    copies = [
        pltpu.make_async_copy(a.at[pl.ds(i * size, size)], b.at[pl.ds(i * size, size)], sems.at[k, i])
        for k, (a, b) in enumerate(((held, new_momentum), (fresh, new_weights)))
        for i in range(pieces)
    ]
    for copy in copies:
        copy.start()
    for copy in copies:
        copy.wait()


def solution(mesh):
    shards, models = mesh.shape["shard"], mesh.shape["model"]

    def folded(x):
        mats, two, wide = x.shape
        x = x.reshape(mats, two, wide // LANES, LANES).transpose(0, 2, 1, 3)
        return x.reshape(shards, mats // (shards * PAIR), ROWS, LANES)

    def unfolded(x, like):
        mats, two, wide = like.shape
        x = x.reshape(mats, wide // LANES, two, LANES).transpose(0, 2, 1, 3)
        return x.reshape(like.shape)

    def on_device(grad_stack, moment_stack, weight_stack):
        grad, moment, weight = folded(grad_stack), folded(moment_stack), folded(weight_stack)
        shape = grad.shape
        chunks = shape[1]
        side, wide = 2 * shards, TILE // 2 * LANES
        near, far = 8, shards // 8
        vmem = pl.BlockSpec(memory_space=pltpu.VMEM)
        hbm = pl.BlockSpec(memory_space=pltpu.HBM)
        block = jax.ShapeDtypeStruct(shape, F32)
        fresh, held = pl.pallas_call(
            functools.partial(exchange_kernel, shards, models, chunks),
            name="exchange",
            out_shape=(block, block),
            in_specs=[hbm, hbm, hbm],
            out_specs=(vmem, vmem),
            scratch_shapes=[
                pltpu.VMEM(shape, F32),
                pltpu.VMEM(shape, F32),
                pltpu.VMEM(shape, F32),
                pltpu.VMEM((chunks, near, far * ROWS, LANES), F32),
                pltpu.VMEM((chunks, shards * ROWS, LANES), F32),
                pltpu.VMEM((chunks, PAIR, side, wide), F32),
                pltpu.VMEM((chunks, PAIR, side, wide), F32),
                pltpu.VMEM((chunks, shards * ROWS, LANES), F32),
                pltpu.VMEM((chunks, near, far * ROWS, LANES), F32),
                pltpu.VMEM((chunks, far, near, ROWS, LANES), F32),
                pltpu.VMEM((2, chunks, models, PAIR, side, side), F32),
                pltpu.SemaphoreType.DMA((3, chunks)),
                pltpu.SemaphoreType.DMA,
                pltpu.SemaphoreType.DMA((chunks,)),
                pltpu.SemaphoreType.DMA,
                pltpu.SemaphoreType.DMA((chunks,)),
                pltpu.SemaphoreType.DMA,
                pltpu.SemaphoreType.DMA((2, chunks)),
                pltpu.SemaphoreType.DMA,
                pltpu.SemaphoreType.DMA((chunks,)),
                pltpu.SemaphoreType.DMA,
                pltpu.SemaphoreType.DMA((chunks,)),
            ],
            compiler_params=pltpu.CompilerParams(
                collective_id=0, has_side_effects=True, vmem_limit_bytes=48 * 1024 * 1024
            ),
        )(grad, moment, weight)
        new_weights, new_momentum = pl.pallas_call(
            write_kernel,
            name="write",
            out_shape=(block, block),
            in_specs=[vmem, vmem],
            out_specs=(hbm, hbm),
            scratch_shapes=[pltpu.SemaphoreType.DMA((2, 4))],
            compiler_params=pltpu.CompilerParams(vmem_limit_bytes=16 * 1024 * 1024),
        )(fresh, held)
        return unfolded(new_weights, weight_stack), unfolded(new_momentum, weight_stack)

    spec = P(None, "shard", "model")
    return jax.shard_map(on_device, mesh=mesh, in_specs=(spec,) * 3, out_specs=(spec,) * 2, check_vma=False)
```
